32 devices in a mesh: dp: 2 (over x), tp: 4 (over z), sp: 4 (over y, core).
Axes of the slice: x: 2, y: 2, z: 4, core: 2. Of those that a mesh axis runs over, the one named last changes fastest.
Arguments:
- x: bfloat16 [6, 512, 3072], P('dp'), parts along dimension 0
- prior_len: int32 [6], P('dp'), parts along dimension 0
- ln_gain: bfloat16 [2, 3072], replicated
- w_query: bfloat16 [2, 3072, 3072], P(None, None, 'tp')
- w_key: bfloat16 [2, 3072, 1024], P(None, None, 'tp')
- w_value: bfloat16 [2, 3072, 1024], P(None, None, 'tp')
- w_out: bfloat16 [2, 3072, 3072], P(None, 'tp')
- w_gate: bfloat16 [2, 3072, 8192], P(None, None, 'tp')
- w_up: bfloat16 [2, 3072, 8192], P(None, None, 'tp')
- w_down: bfloat16 [2, 8192, 3072], P(None, 'tp')
- swa_k: bfloat16 [6, 4096, 8, 128], P('dp', None, 'tp'), parts along dimension 0
- swa_v: bfloat16 [6, 4096, 8, 128], P('dp', None, 'tp'), parts along dimension 0
- glb_k: bfloat16 [6, 16384, 8, 128], P('dp', 'sp', 'tp'), parts along dimension 0
- glb_v: bfloat16 [6, 16384, 8, 128], P('dp', 'sp', 'tp'), parts along dimension 0
Outputs:
- output 1: bfloat16 [6, 512, 3072], P('dp'), parts along dimension 0
- output 2: bfloat16 [6, 4096, 8, 128], P('dp', None, 'tp'), parts along dimension 0
- output 3: bfloat16 [6, 4096, 8, 128], P('dp', None, 'tp'), parts along dimension 0
- output 4: bfloat16 [6, 16384, 8, 128], P('dp', 'sp', 'tp'), parts along dimension 0
- output 5: bfloat16 [6, 16384, 8, 128], P('dp', 'sp', 'tp'), parts along dimension 0
There are 2 independent parts. The reference program is written for one: setup_inputs(seed, part) draws one part's arguments, and reference() takes and returns one part's arrays. A program takes and returns all parts, laid end to end along the dimension named above; an argument that names none is the same for every part.
All inputs are finite; a program needn't handle non-finite values.
Results may differ from the reference program's by a relative error of at most 0.010961.
Values sent between devices are 32-bit elements.
A program may use at most 1 GiB of HBM per device.

```python
import math
import jax
import jax.numpy as jnp
from jax import lax

BATCH_ROWS = 3
CHUNK_LEN = 512
MODEL_DIM = 3072
NUM_HEADS = 24
KV_HEADS = 8
FFN_DIM = 8192
HEAD_DIM = 128
WINDOW = 4096
SHARD_LEN = 4096
CACHE_LEN = 16384
ROPE_BASE = 50000

GROUP_SIZE = NUM_HEADS // KV_HEADS
SHARD_COUNT = CACHE_LEN // SHARD_LEN
NORM_EPS = 1e-5


def draw_prior(rng_key):
    key_rows, key_shard = jax.random.split(rng_key)
    lengths = jax.random.randint(key_rows, (BATCH_ROWS,), WINDOW, CACHE_LEN - CHUNK_LEN + 1)
    low_shard = (WINDOW + CHUNK_LEN // 2 + SHARD_LEN - 1) // SHARD_LEN
    boundary = jax.random.randint(key_shard, (), low_shard, SHARD_COUNT)
    lengths = lengths.at[0].set(CACHE_LEN - CHUNK_LEN)
    lengths = lengths.at[1].set(boundary * SHARD_LEN - CHUNK_LEN // 2)
    return lengths.astype(jnp.int32)


def gauss_draw(rng_key, draw_shape, draw_scale):
    return (jax.random.normal(rng_key, draw_shape, jnp.float32) * draw_scale).astype(jnp.bfloat16)


def setup_inputs(seed: int = 0, part: int = 0) -> dict:
    root_key = jax.random.key(seed)
    shared = jax.random.split(root_key, 8)
    own_keys = jax.random.split(jax.random.fold_in(root_key, part), 6)
    q_width = NUM_HEADS * HEAD_DIM
    kv_width = KV_HEADS * HEAD_DIM
    query_scale = jnp.array([math.sqrt(math.log(WINDOW / 4.0)), math.sqrt(math.log(CACHE_LEN / 4.0))], jnp.float32)[:, None, None] / math.sqrt(MODEL_DIM)
    swa_shape = (BATCH_ROWS, WINDOW, KV_HEADS, HEAD_DIM)
    glb_shape = (BATCH_ROWS, CACHE_LEN, KV_HEADS, HEAD_DIM)
    return {
        'x': gauss_draw(own_keys[0], (BATCH_ROWS, CHUNK_LEN, MODEL_DIM), 1.0),
        'prior_len': draw_prior(own_keys[1]),
        'ln_gain': (1.0 + 0.25 * jax.random.normal(shared[0], (2, MODEL_DIM), jnp.float32)).astype(jnp.bfloat16),
        'w_query': gauss_draw(shared[1], (2, MODEL_DIM, q_width), query_scale),
        'w_key': gauss_draw(shared[2], (2, MODEL_DIM, kv_width), MODEL_DIM ** -0.5),
        'w_value': gauss_draw(shared[3], (2, MODEL_DIM, kv_width), MODEL_DIM ** -0.5),
        'w_out': gauss_draw(shared[4], (2, q_width, MODEL_DIM), q_width ** -0.5),
        'w_gate': gauss_draw(shared[5], (2, MODEL_DIM, FFN_DIM), MODEL_DIM ** -0.5),
        'w_up': gauss_draw(shared[6], (2, MODEL_DIM, FFN_DIM), MODEL_DIM ** -0.5),
        'w_down': gauss_draw(shared[7], (2, FFN_DIM, MODEL_DIM), FFN_DIM ** -0.5),
        'swa_k': gauss_draw(own_keys[2], swa_shape, 1.0),
        'swa_v': gauss_draw(own_keys[3], swa_shape, 1.0),
        'glb_k': gauss_draw(own_keys[4], glb_shape, 1.0),
        'glb_v': gauss_draw(own_keys[5], glb_shape, 1.0),
    }


def layer_norm(hidden, norm_gain):
    as_float = hidden.astype(jnp.float32)
    centered = as_float - jnp.mean(as_float, axis=-1, keepdims=True)
    variance = jnp.mean(centered * centered, axis=-1, keepdims=True)
    return (centered * lax.rsqrt(variance + NORM_EPS) * norm_gain.astype(jnp.float32)).astype(jnp.bfloat16)


def rotate_pairs(vectors, positions):
    inv_freq = ROPE_BASE ** (-jnp.arange(0, HEAD_DIM, 2).astype(jnp.float32) / HEAD_DIM)
    angles = positions.astype(jnp.float32)[..., None] * inv_freq
    cosine = jnp.cos(angles)[..., None, :]
    sine_val = jnp.sin(angles)[..., None, :]
    pairs = vectors.astype(jnp.float32).reshape(vectors.shape[:-1] + (HEAD_DIM // 2, 2))
    even_part = pairs[..., 0]
    odd_part = pairs[..., 1]
    turned = jnp.stack([even_part * cosine - odd_part * sine_val, odd_part * cosine + even_part * sine_val], axis=-1)
    return turned.reshape(vectors.shape).astype(jnp.bfloat16)


def attend_row(queries, keys, values, allowed):
    def one_head(head_idx):
        kv_idx = head_idx // GROUP_SIZE
        q_head = lax.dynamic_index_in_dim(queries, head_idx, axis=1, keepdims=False)
        k_head = lax.dynamic_index_in_dim(keys, kv_idx, axis=1, keepdims=False)
        v_head = lax.dynamic_index_in_dim(values, kv_idx, axis=1, keepdims=False)
        scores = jnp.dot(q_head, k_head.T, preferred_element_type=jnp.float32) * HEAD_DIM ** -0.5
        scores = jnp.where(allowed, scores, -jnp.inf)
        weights = jnp.exp(scores - jnp.max(scores, axis=1, keepdims=True))
        denominator = jnp.sum(weights, axis=1, keepdims=True)
        numerator = jnp.dot(weights.astype(jnp.bfloat16), v_head, preferred_element_type=jnp.float32)
        return (numerator / denominator).astype(jnp.bfloat16)
    per_head = lax.map(one_head, jnp.arange(NUM_HEADS))
    return jnp.transpose(per_head, (1, 0, 2))


def take_rows(source, index_row):
    return jnp.take(source, index_row, axis=0)


def write_row(cache_row, fresh_row, first_pos):
    return lax.dynamic_update_slice_in_dim(cache_row, fresh_row, first_pos, axis=0)


def reference(x, prior_len, ln_gain, w_query, w_key, w_value, w_out, w_gate, w_up, w_down, swa_k, swa_v, glb_k, glb_v):
    tokens = BATCH_ROWS * CHUNK_LEN
    positions = prior_len[:, None] + jnp.arange(CHUNK_LEN)[None, :]

    def project(hidden, layer_idx):
        flat_in = layer_norm(hidden, ln_gain[layer_idx]).reshape(tokens, MODEL_DIM)
        queries = jnp.dot(flat_in, w_query[layer_idx], preferred_element_type=jnp.float32).astype(jnp.bfloat16)
        fresh_k = jnp.dot(flat_in, w_key[layer_idx], preferred_element_type=jnp.float32).astype(jnp.bfloat16)
        fresh_v = jnp.dot(flat_in, w_value[layer_idx], preferred_element_type=jnp.float32).astype(jnp.bfloat16)
        gate_act = jnp.dot(flat_in, w_gate[layer_idx], preferred_element_type=jnp.float32)
        up_act = jnp.dot(flat_in, w_up[layer_idx], preferred_element_type=jnp.float32)
        mlp_mid = (jax.nn.silu(gate_act) * up_act).astype(jnp.bfloat16)
        mlp_out = jnp.dot(mlp_mid, w_down[layer_idx], preferred_element_type=jnp.float32)
        return (queries.reshape(BATCH_ROWS, CHUNK_LEN, NUM_HEADS, HEAD_DIM),
                fresh_k.reshape(BATCH_ROWS, CHUNK_LEN, KV_HEADS, HEAD_DIM),
                fresh_v.reshape(BATCH_ROWS, CHUNK_LEN, KV_HEADS, HEAD_DIM),
                mlp_out)

    def finish(hidden, attended, mlp_out, layer_idx):
        attn_out = jnp.dot(attended.reshape(tokens, NUM_HEADS * HEAD_DIM), w_out[layer_idx], preferred_element_type=jnp.float32)
        total = hidden.reshape(tokens, MODEL_DIM).astype(jnp.float32) + attn_out + mlp_out
        return total.astype(jnp.bfloat16).reshape(BATCH_ROWS, CHUNK_LEN, MODEL_DIM)

    queries, fresh_k, fresh_v, mlp_out = project(x, 0)
    queries = rotate_pairs(queries, positions)
    fresh_k = rotate_pairs(fresh_k, positions)
    slot_ids = jnp.arange(WINDOW)
    last_pos = prior_len[:, None] - 1
    slot_pos = last_pos - jnp.mod(last_pos - slot_ids[None, :], WINDOW)
    key_pos = jnp.concatenate([slot_pos, positions], axis=1)
    allowed = (key_pos[:, None, :] <= positions[:, :, None]) & (key_pos[:, None, :] > positions[:, :, None] - WINDOW)

    def sliding_row(row_args):
        q_row, k_row, v_row, kc_row, vc_row, allow_row = row_args
        return attend_row(q_row, jnp.concatenate([kc_row, k_row], axis=0), jnp.concatenate([vc_row, v_row], axis=0), allow_row)

    attended = lax.map(sliding_row, (queries, fresh_k, fresh_v, swa_k, swa_v, allowed))
    hidden = finish(x, attended, mlp_out, 0)
    slot_offsets = jnp.mod(slot_ids[None, :] - prior_len[:, None], WINDOW)
    fresh_slot = (slot_offsets < CHUNK_LEN)[:, :, None, None]
    pick = jnp.minimum(slot_offsets, CHUNK_LEN - 1)
    swa_k_new = jnp.where(fresh_slot, jax.vmap(take_rows)(fresh_k, pick), swa_k)
    swa_v_new = jnp.where(fresh_slot, jax.vmap(take_rows)(fresh_v, pick), swa_v)

    queries, fresh_k, fresh_v, mlp_out = project(hidden, 1)
    glb_k_new = jax.vmap(write_row)(glb_k, fresh_k, prior_len)
    glb_v_new = jax.vmap(write_row)(glb_v, fresh_v, prior_len)
    cache_pos = jnp.arange(CACHE_LEN)

    def global_row(row_args):
        q_row, kc_row, vc_row, pos_row = row_args
        return attend_row(q_row, kc_row, vc_row, cache_pos[None, :] <= pos_row[:, None])

    attended = lax.map(global_row, (queries, glb_k_new, glb_v_new, positions))
    result = finish(hidden, attended, mlp_out, 1)
    return (result, swa_k_new, swa_v_new, glb_k_new, glb_v_new)
```

```python
import functools
import math

import jax
import jax.numpy as jnp
from jax import lax
from jax.experimental import pallas as pl
from jax.experimental.pallas import tpu as pltpu
from jax.sharding import PartitionSpec as P

HEAD_DIM = 128
ROPE_BASE = 50000
NORM_EPS = 1e-5
WINDOW = 4096
SHARD = 4096
CHUNK = 512
OWN = 128
BK = 1024
NEG = -1e30
LOG2E_SCALE = math.log2(math.e) / math.sqrt(HEAD_DIM)
MESH = pl.DeviceIdType.MESH


def layer_norm(hidden, norm_gain):
    as_float = hidden.astype(jnp.float32)
    centered = as_float - jnp.mean(as_float, axis=-1, keepdims=True)
    variance = jnp.mean(centered * centered, axis=-1, keepdims=True)
    return (centered * lax.rsqrt(variance + NORM_EPS) * norm_gain.astype(jnp.float32)).astype(jnp.bfloat16)


def rope_tables(prior_row):
    lane = lax.broadcasted_iota(jnp.int32, (1, HEAD_DIM), 1)
    inv_freq = ROPE_BASE ** (-((lane // 2) * 2).astype(jnp.float32) / HEAD_DIM)
    positions = (prior_row + jnp.arange(CHUNK, dtype=jnp.int32)).astype(jnp.float32)
    angles = positions[:, None] * inv_freq
    return jnp.cos(angles), jnp.where(lane % 2 == 0, -jnp.sin(angles), jnp.sin(angles))


def rotate(vec, cosine, sine):
    lane = lax.broadcasted_iota(jnp.int32, vec.shape, 1)
    swapped = jnp.where(lane % 2 == 0, pltpu.roll(vec, HEAD_DIM - 1, 1), pltpu.roll(vec, 1, 1))
    return vec * cosine + swapped * sine


def attention_body(row, glb, width, info, ins, kc_ref, vc_ref, outs, ko_ref, vo_ref, scr):
    (qt, acc, mx, sm, alpha, inter, kg, vt, fk, fvt, padk, padv, s0, s1, p0, p1) = scr
    step = pl.program_id(0)
    tiles = qt.shape[0]
    per_g = tiles // 2
    start_rel = info[0]
    first_tok = info[1]

    def tile_g(t):
        return t // per_g if per_g > 1 else t

    def put_fresh(pad, g, block, val):
        pad[pl.ds(2 * BK + 2 * block * OWN + g, val.shape[0], stride=2), :] = val

    def process(nk, k_src, vt_src, mask_fn):
        def qk(t, s_ref):
            s = jnp.dot(k_src[tile_g(t), :nk, :], qt[t], preferred_element_type=jnp.float32)
            if mask_fn is not None:
                s = jnp.where(mask_fn(t, nk), s, NEG)
            s_ref[:nk, :] = s
            slot = 0 if s_ref is s0 else 1
            alpha[slot, 1:2, :] = jnp.max(s, axis=0, keepdims=True)

        def soft(t, slot, s_ref, p_ref):
            old = mx[t, 0:1, :]
            new = jnp.maximum(old, alpha[slot, 1:2, :])
            e = jnp.exp2((s_ref[:nk, :] - new) * LOG2E_SCALE)
            fade = jnp.exp2((old - new) * LOG2E_SCALE)
            sm[t, 0:1, :] = sm[t, 0:1, :] * fade + jnp.sum(e, axis=0, keepdims=True)
            mx[t, 0:1, :] = new
            alpha[slot, 0:1, :] = fade
            p_ref[:nk, :] = e.astype(jnp.bfloat16)

        def pv(t, slot, p_ref):
            add = jnp.dot(vt_src[tile_g(t), :, :nk], p_ref[:nk, :], preferred_element_type=jnp.float32)
            acc[t] = acc[t] * alpha[slot, 0:1, :] + add

        qk(0, s0)
        pairs = tiles // 2
        if pairs == 1:
            qk(1, s1)
            soft(0, 0, s0, p0)
            pv(0, 0, p0)
            soft(1, 1, s1, p1)
            pv(1, 1, p1)
        else:
            qk(1, s1)
            soft(0, 0, s0, p0)

            def body(i, _):
                t = 2 * i
                qk(t + 2, s0)
                soft(t + 1, 1, s1, p1)
                pv(t, 0, p0)
                qk(t + 3, s1)
                soft(t + 2, 0, s0, p0)
                pv(t + 1, 1, p1)
                return 0

            lax.fori_loop(0, pairs - 1, body, 0)
            soft(tiles - 1, 1, s1, p1)
            pv(tiles - 2, 0, p0)
            pv(tiles - 1, 1, p1)

    def tok_of(t):
        lane = lax.broadcasted_iota(jnp.int32, (1, width), 1)
        if glb:
            return lane + (t % 2) * width
        return lax.rem(lane, OWN) + first_tok

    def fresh_mask(t, nk):
        key = lax.broadcasted_iota(jnp.int32, (nk, width), 0)
        ok = key <= tok_of(t)
        if glb:
            pos = lax.broadcasted_iota(jnp.int32, (nk, 1), 0) + start_rel
            ok = ok & (pos >= 0) & (pos < SHARD)
        return ok

    @pl.when(step == 0)
    def _():
        mx[...] = jnp.full_like(mx, NEG)
        sm[...] = jnp.zeros_like(sm)
        acc[...] = jnp.zeros_like(acc)

        def put_q(h, block, val):
            g, j = divmod(h, 3)
            turned = val.T.astype(jnp.bfloat16)
            if glb:
                base = g * 6 + j * 2
                for b in range(4):
                    @pl.when(block == b)
                    def _(b=b):
                        qt[base + b // 2, :, (b % 2) * OWN:(b % 2 + 1) * OWN] = turned
            else:
                qt[g, :, j * OWN:(j + 1) * OWN] = turned

        def put_kv(g, block, kval, vval):
            put_fresh(padk, g, block, kval)
            put_fresh(padv, g, block, vval)
            fk[g, pl.ds(pl.multiple_of(block * OWN, OWN), OWN), :] = kval.astype(jnp.bfloat16)
            turned = vval.T.astype(jnp.bfloat16)
            for b in range(4):
                @pl.when(block == b)
                def _(b=b):
                    fvt[g, :, b * OWN:(b + 1) * OWN] = turned

        if glb:
            me = info[2]
            order = (me, me ^ 2, me ^ 1, me ^ 3)
            for src, block in zip(ins, order):
                for h in range(6):
                    put_q(h, block, src[:, h * HEAD_DIM:(h + 1) * HEAD_DIM])
                for g in range(2):
                    k0 = 6 * HEAD_DIM + g * HEAD_DIM
                    v0 = 8 * HEAD_DIM + g * HEAD_DIM
                    put_kv(g, block, src[:, k0:k0 + HEAD_DIM].astype(jnp.bfloat16).astype(jnp.float32),
                           src[:, v0:v0 + HEAD_DIM].astype(jnp.bfloat16).astype(jnp.float32))
        else:
            q_ref, k_ref, v_ref, cos_ref, sin_ref = ins
            at = pl.ds(pl.multiple_of(first_tok, OWN), OWN)
            for h in range(6):
                val = q_ref[:, h * HEAD_DIM:(h + 1) * HEAD_DIM].astype(jnp.float32)
                put_q(h, 0, rotate(val, cos_ref[at, :], sin_ref[at, :]))
            for g in range(2):
                for b in range(4):
                    rows = slice(b * OWN, (b + 1) * OWN)
                    cols = slice(g * HEAD_DIM, (g + 1) * HEAD_DIM)
                    kval = rotate(k_ref[rows, cols].astype(jnp.float32), cos_ref[rows, :], sin_ref[rows, :])
                    kval = kval.astype(jnp.bfloat16).astype(jnp.float32)
                    vval = v_ref[rows, cols].astype(jnp.float32)
                    put_fresh(padk, g, b, kval)
                    put_fresh(padv, g, b, vval)
                    fk[g, rows, :] = kval.astype(jnp.bfloat16)
                    fvt[g, :, rows] = vval.T.astype(jnp.bfloat16)

        if glb:
            @pl.when((start_rel > -CHUNK) & (start_rel < SHARD))
            def _():
                process(CHUNK, fk, fvt, fresh_mask)
        else:
            process(CHUNK, fk, fvt, fresh_mask)

    first_key = step * BK
    if glb:
        shift = first_key - start_rel
    else:
        shift = first_key - start_rel
        shift = jnp.where(shift >= WINDOW // 2, shift - WINDOW, shift)
        shift = jnp.where(shift < -(WINDOW // 2), shift + WINDOW, shift)
    touched = (shift > -BK) & (shift < CHUNK)

    @pl.when(jnp.logical_not(touched))
    def _():
        ko_ref[0] = kc_ref[0]
        vo_ref[0] = vc_ref[0]

    @pl.when(touched)
    def _():
        token = lax.broadcasted_iota(jnp.int32, (2 * BK, 1), 0) // 2 + shift
        inside = (token >= 0) & (token < CHUNK)
        at = pl.ds(2 * BK + 2 * shift, 2 * BK)
        ko_ref[0] = jnp.where(inside, padk[at, :], kc_ref[0].astype(jnp.float32)).astype(jnp.bfloat16)
        vo_ref[0] = jnp.where(inside, padv[at, :], vc_ref[0].astype(jnp.float32)).astype(jnp.bfloat16)

    def split_heads():
        inter[...] = kc_ref[0].astype(jnp.float32)
        for g in range(2):
            kg[g] = inter[pl.ds(g, BK, stride=2), :].astype(jnp.bfloat16)
        inter[...] = vc_ref[0].astype(jnp.float32)
        for g in range(2):
            vt[g] = inter[pl.ds(g, BK, stride=2), :].T.astype(jnp.bfloat16)

    if glb:
        def old_mask(t, nk):
            del t
            return lax.broadcasted_iota(jnp.int32, (nk, 1), 0) < start_rel - first_key

        @pl.when(first_key < start_rel)
        def _():
            split_heads()

            @pl.when(first_key + BK <= start_rel)
            def _():
                process(BK, kg, vt, None)

            @pl.when(first_key + BK > start_rel)
            def _():
                process(BK, kg, vt, old_mask)
    else:
        def old_mask(t, nk):
            token = lax.broadcasted_iota(jnp.int32, (nk, width), 0) + shift
            return (token < 0) | (token > tok_of(t))

        split_heads()

        @pl.when(touched)
        def _():
            process(BK, kg, vt, old_mask)

        @pl.when(jnp.logical_not(touched))
        def _():
            process(BK, kg, vt, None)

    @pl.when(step == pl.num_programs(0) - 1)
    def _():
        if not glb:
            (att_ref,) = outs
            for g in range(2):
                for j in range(3):
                    cols = slice(j * OWN, (j + 1) * OWN)
                    done = acc[g, :, cols] / sm[g, 0:1, cols]
                    h = 3 * g + j
                    att_ref[:, h * HEAD_DIM:(h + 1) * HEAD_DIM] = done.T.astype(jnp.bfloat16)
        else:
            keep_ref, send_ref = outs
            core_is_0 = first_tok == 0
            row_id = lax.broadcasted_iota(jnp.int32, (HEAD_DIM, OWN), 0)
            for half in range(2):
                stats = [jnp.zeros((HEAD_DIM, OWN), jnp.float32) for _ in range(2)]
                for h in range(6):
                    g, j = divmod(h, 3)
                    t = g * 6 + j * 2 + half
                    vals = []
                    for c in range(2):
                        cols = slice(c * OWN, (c + 1) * OWN)
                        vals.append(acc[t, :, cols].T)
                        stats[c] = jnp.where(row_id == h, mx[t, 0:1, cols] * LOG2E_SCALE, stats[c])
                        stats[c] = jnp.where(row_id == 8 + h, sm[t, 0:1, cols], stats[c])
                    cols = slice(h * HEAD_DIM, (h + 1) * HEAD_DIM)
                    keep_ref[half, :, cols] = jnp.where(core_is_0, vals[0], vals[1])
                    send_ref[half, :, cols] = jnp.where(core_is_0, vals[1], vals[0])
                last = slice(6 * HEAD_DIM, 7 * HEAD_DIM)
                s_a, s_b = stats[0].T, stats[1].T
                keep_ref[half, :, last] = jnp.where(core_is_0, s_a, s_b)
                send_ref[half, :, last] = jnp.where(core_is_0, s_b, s_a)


def attention(row, glb, info, ins, cache_k, cache_v, prev):
    width = 256 if glb else 3 * OWN
    tiles = 12 if glb else 2
    n_in = len(ins)
    n_prev = 0 if prev is None else 2
    cache_spec = pl.BlockSpec((1, 2 * BK, HEAD_DIM), lambda i, info: (row, i, 0))

    def kernel(info, *refs):
        in_refs = refs[:n_in]
        kc_ref, vc_ref = refs[n_in:n_in + 2]
        rest = refs[n_in + 2 + n_prev:]
        n_out = 2 if glb else 1
        attention_body(row, glb, width, info, in_refs, kc_ref, vc_ref, rest[:n_out], rest[n_out], rest[n_out + 1],
                       rest[n_out + 2:])

    whole = [pl.BlockSpec(a.shape, lambda i, info, n=a.ndim: (0,) * n) for a in ins]
    if glb:
        outs = [jax.ShapeDtypeStruct((2, OWN, 7 * HEAD_DIM), jnp.float32)] * 2
    else:
        outs = [jax.ShapeDtypeStruct((OWN, 6 * HEAD_DIM), jnp.bfloat16)]
    out_specs = [pl.BlockSpec(o.shape, lambda i, info, n=len(o.shape): (0,) * n) for o in outs]
    cache_out = jax.ShapeDtypeStruct(cache_k.shape, cache_k.dtype)
    f32, bf16 = jnp.float32, jnp.bfloat16
    scratch = [
        pltpu.VMEM((tiles, HEAD_DIM, width), bf16),
        pltpu.VMEM((tiles, HEAD_DIM, width), f32),
        pltpu.VMEM((tiles, 8, width), f32),
        pltpu.VMEM((tiles, 8, width), f32),
        pltpu.VMEM((2, 8, width), f32),
        pltpu.VMEM((2 * BK, HEAD_DIM), f32),
        pltpu.VMEM((2, BK, HEAD_DIM), bf16),
        pltpu.VMEM((2, HEAD_DIM, BK), bf16),
        pltpu.VMEM((2, CHUNK, HEAD_DIM), bf16),
        pltpu.VMEM((2, HEAD_DIM, CHUNK), bf16),
        pltpu.VMEM((4 * BK + 2 * CHUNK, HEAD_DIM), f32),
        pltpu.VMEM((4 * BK + 2 * CHUNK, HEAD_DIM), f32),
        pltpu.VMEM((BK, width), f32),
        pltpu.VMEM((BK, width), f32),
        pltpu.VMEM((BK, width), bf16),
        pltpu.VMEM((BK, width), bf16),
    ]
    keys = SHARD + CHUNK
    flops = 4 * tiles * width * keys * HEAD_DIM
    call = pl.pallas_call(
        kernel,
        grid_spec=pltpu.PrefetchScalarGridSpec(
            num_scalar_prefetch=1,
            grid=(SHARD // BK,),
            in_specs=whole + [cache_spec, cache_spec] + [pl.BlockSpec(memory_space=pl.ANY)] * n_prev,
            out_specs=out_specs + [cache_spec, cache_spec],
            scratch_shapes=scratch,
        ),
        out_shape=outs + [cache_out, cache_out],
        input_output_aliases={} if prev is None else {1 + n_in + 2: len(outs), 1 + n_in + 3: len(outs) + 1},
        compiler_params=pltpu.CompilerParams(dimension_semantics=("arbitrary",), vmem_limit_bytes=48 << 20),
        cost_estimate=pl.CostEstimate(flops=flops, transcendentals=tiles * width * keys, bytes_accessed=12 << 20),
        name="global_rows" if glb else "sliding_rows",
    )
    return call(info, *ins, cache_k, cache_v, *(() if prev is None else prev))


def merge_pair(a, b, normalise):
    lane = lax.broadcasted_iota(jnp.int32, (a.shape[0], HEAD_DIM), 1)
    sa, sb = a[:, 6 * HEAD_DIM:], b[:, 6 * HEAD_DIM:]
    stats = jnp.zeros_like(sa)
    heads = []
    for h in range(6):
        ma, mb = sa[:, h:h + 1], sb[:, h:h + 1]
        la, lb = sa[:, 8 + h:9 + h], sb[:, 8 + h:9 + h]
        top = jnp.maximum(ma, mb)
        fa, fb = jnp.exp2(ma - top), jnp.exp2(mb - top)
        total = la * fa + lb * fb
        cols = slice(h * HEAD_DIM, (h + 1) * HEAD_DIM)
        val = a[:, cols] * fa + b[:, cols] * fb
        if normalise:
            val = val / total
        heads.append(val)
        stats = jnp.where(lane == h, top, jnp.where(lane == 8 + h, total, stats))
    return heads, stats


def merge_cores(info, keep, recv):
    def kernel(info, keep_ref, recv_ref, keep_out, send_out):
        for half in range(2):
            heads, stats = merge_pair(keep_ref[half], recv_ref[half], False)
            mine = info[0] == half
            for dst, cond in ((keep_out, mine), (send_out, jnp.logical_not(mine))):
                @pl.when(cond)
                def _(dst=dst):
                    for h in range(6):
                        dst[:, h * HEAD_DIM:(h + 1) * HEAD_DIM] = heads[h]
                    dst[:, 6 * HEAD_DIM:] = stats

    shape = jax.ShapeDtypeStruct((OWN, 7 * HEAD_DIM), jnp.float32)
    vmem = pl.BlockSpec(memory_space=pltpu.VMEM)
    return pl.pallas_call(
        kernel,
        in_specs=[pl.BlockSpec(memory_space=pltpu.SMEM), vmem, vmem],
        out_specs=[vmem, vmem],
        out_shape=[shape, shape],
        cost_estimate=pl.CostEstimate(flops=1 << 30, transcendentals=1 << 12, bytes_accessed=3 << 20),
        name="merge_cores",
    )(info, keep, recv)


def merge_last(keep, recv):
    def kernel(keep_ref, recv_ref, out_ref):
        heads, _ = merge_pair(keep_ref[...], recv_ref[...], True)
        for h in range(6):
            out_ref[:, h * HEAD_DIM:(h + 1) * HEAD_DIM] = heads[h].astype(jnp.bfloat16)

    vmem = pl.BlockSpec(memory_space=pltpu.VMEM)
    return pl.pallas_call(
        kernel,
        in_specs=[vmem, vmem],
        out_specs=vmem,
        out_shape=jax.ShapeDtypeStruct((OWN, 6 * HEAD_DIM), jnp.bfloat16),
        cost_estimate=pl.CostEstimate(flops=1 << 30, transcendentals=1 << 12, bytes_accessed=1 << 20),
        name="merge_last",
    )(keep, recv)


def dot32(a, b):
    return jnp.dot(a, b, preferred_element_type=jnp.float32)


def swap(value, bit):
    return lax.ppermute(value, 'sp', [(i, i ^ bit) for i in range(4)])


def scope(name):
    return jax.named_scope(name)


def norm_and_keys(me, x, gain, w_key, w_value):
    rows, chunk, model = x.shape
    kv = w_key.shape[1]

    def kernel(me_ref, x_ref, gain_ref, wk_ref, wv_ref, own_ref, k_ref, v_ref, wkv):
        block = pl.program_id(1)

        @pl.when((pl.program_id(0) == 0) & (block == 0))
        def _():
            wkv[:, :kv] = wk_ref[...]
            wkv[:, kv:] = wv_ref[...]

        normed = layer_norm(x_ref[0], gain_ref[...])

        @pl.when(block == me_ref[0])
        def _():
            own_ref[...] = normed

        both = jnp.dot(normed, wkv[...], preferred_element_type=jnp.float32).astype(jnp.bfloat16)
        k_ref[...] = both[:, :kv]
        v_ref[...] = both[:, kv:]

    blocks = chunk // OWN
    return pl.pallas_call(
        kernel,
        grid_spec=pltpu.PrefetchScalarGridSpec(
            num_scalar_prefetch=1,
            grid=(rows, blocks),
            in_specs=[
                pl.BlockSpec((1, OWN, model), lambda r, i, me: (r, i, 0)),
                pl.BlockSpec((1, model), lambda r, i, me: (0, 0)),
                pl.BlockSpec((model, kv), lambda r, i, me: (0, 0)),
                pl.BlockSpec((model, kv), lambda r, i, me: (0, 0)),
            ],
            out_specs=[
                pl.BlockSpec((OWN, model), lambda r, i, me: (r, 0)),
                pl.BlockSpec((OWN, kv), lambda r, i, me: (r * blocks + i, 0)),
                pl.BlockSpec((OWN, kv), lambda r, i, me: (r * blocks + i, 0)),
            ],
            scratch_shapes=[pltpu.VMEM((model, 2 * kv), jnp.bfloat16)],
        ),
        out_shape=[
            jax.ShapeDtypeStruct((rows * OWN, model), jnp.bfloat16),
            jax.ShapeDtypeStruct((rows * chunk, kv), jnp.bfloat16),
            jax.ShapeDtypeStruct((rows * chunk, kv), jnp.bfloat16),
        ],
        compiler_params=pltpu.CompilerParams(dimension_semantics=("arbitrary", "arbitrary"), vmem_limit_bytes=40 << 20),
        cost_estimate=pl.CostEstimate(flops=4 * rows * chunk * model * kv, transcendentals=0, bytes_accessed=16 << 20),
        name="norm_and_keys",
    )(me, x, gain, w_key, w_value)


PIECE = 64
COLS = 512
WSLOTS = 3
RB_LAG = 3
END_LAG = 9
Y_LAG = 12
B_LAG = 2


def line_sum(last, layer, att, mid, own, w_out, w_down, rows):
    tokens, model = own.shape
    width, inner = att.shape[1], mid.shape[1]
    ncol = model // COLS
    pieces = (tokens // PIECE) * ncol
    per_row = (OWN // PIECE) * ncol
    groups = pieces // 2
    copies_y = 3 if last else 0

    def kernel(att_ref, mid_ref, own_ref, wo_hbm, wd_hbm, out_ref, wo, wd, wsem, mine, edge, cross, s1, r1, s2, r2, s3,
               *more):
        tp, sp = lax.axis_index("tp"), lax.axis_index("sp")
        is_mid = (tp == 1) | (tp == 2)
        is_end = (tp == 0) | (tp == 3)
        inward = {"tp": 1 + tp // 3}
        outward = {"tp": 3 * (tp // 2)}
        partner = {"tp": 3 - tp}
        far = {"sp": (sp + 2) % 4}
        near = {"sp": sp + 1 - 2 * (sp % 2)}
        if last:
            from_y, from_c, from_b, sy, ry, sc, rc, sb, rb = more

        def remote(src, dst, send, recv, to):
            return pltpu.make_async_remote_copy(src, dst, send, recv, device_id=to, device_id_type=MESH)

        def to_mid(j):
            return remote(mine.at[j], edge.at[j], s1.at[j], r1.at[j], inward)

        def across(j):
            return remote(mine.at[j], cross.at[j], s2.at[j], r2.at[j], partner)

        def to_end(j):
            return remote(edge.at[j], edge.at[j], s3.at[j], r1.at[j], outward)

        def to_far(j):
            return remote(edge.at[j], from_y.at[j], sy.at[j], ry.at[j], far)

        def to_near(j):
            return remote(edge.at[j], from_c.at[j], sc.at[j], rc.at[j], near)

        def hand_on(j):
            return remote(from_y.at[j], from_b.at[j], sb.at[j], rb.at[j], near)

        def weights(g):
            n, slot = g % ncol, g % WSLOTS
            cols = pl.ds(pl.multiple_of(n * COLS, COLS), COLS)
            return (pltpu.make_async_copy(wo_hbm.at[layer, :, cols], wo.at[slot], wsem.at[slot, 0]),
                    pltpu.make_async_copy(wd_hbm.at[layer, :, cols], wd.at[slot], wsem.at[slot, 1]))

        def place(j):
            r, rest = j // per_row, j % per_row
            n, half = rest // 2, rest % 2
            return r, half, pl.ds(pl.multiple_of(n * COLS, COLS), COLS)

        for g in range(WSLOTS):
            for copy in weights(g):
                copy.start()

        barrier = pltpu.get_barrier_semaphore()

        def meet(to):
            pl.semaphore_signal(barrier, inc=1, device_id=to, device_id_type=MESH)

        if last:
            meet(far)
            meet(near)

        @pl.when(is_end)
        def _():
            meet(inward)
            pl.semaphore_wait(barrier, 1 + (2 if last else 0))

        @pl.when(is_mid)
        def _():
            meet(outward)
            meet(partner)
            pl.semaphore_wait(barrier, 2 + (2 if last else 0))

        def result(j, val, own_val):
            del own_val
            r, half, cols = place(j)
            if last:
                at = pl.ds(pl.multiple_of(sp * OWN + half * PIECE, PIECE), PIECE)
                out_ref[r, at, cols] = val.astype(out_ref.dtype)
            else:
                at = pl.ds(pl.multiple_of(r * OWN + half * PIECE, PIECE), PIECE)
                out_ref[at, cols] = val.astype(out_ref.dtype)

        def foreign(j, val, owner):
            r, half, cols = place(j)
            at = pl.ds(pl.multiple_of(owner * OWN + half * PIECE, PIECE), PIECE)
            out_ref[r, at, cols] = val.astype(out_ref.dtype)

        def step(q, _):
            @pl.when((q % 2 == 0) & (q < pieces))
            def _():
                g = q // 2
                slot = g % WSLOTS
                for copy in weights(g):
                    copy.wait()
                rows_at = pl.ds(pl.multiple_of((g // ncol) * OWN, OWN), OWN)
                val = jnp.dot(att_ref[rows_at, :], wo[slot], preferred_element_type=jnp.float32)
                val += jnp.dot(mid_ref[rows_at, :], wd[slot], preferred_element_type=jnp.float32)
                mine[q] = val[:PIECE]
                mine[q + 1] = val[PIECE:]

                @pl.when(g + WSLOTS < groups)
                def _():
                    for copy in weights(g + WSLOTS):
                        copy.start()

            @pl.when(is_end)
            def _():
                @pl.when((q >= 4) & (q < pieces + 4))
                def _():
                    to_mid(q - 4).wait_send()

                @pl.when(q < pieces)
                def _():
                    to_mid(q).start()

                @pl.when((q >= END_LAG) & (q < pieces + END_LAG))
                def _():
                    j = q - END_LAG
                    to_end(j).wait_recv()
                    result(j, edge[j], None)
                    if last:
                        to_far(j).start()
                        to_near(j).start()

            @pl.when(is_mid)
            def _():
                @pl.when((q >= 1) & (q < pieces + 1))
                def _():
                    j = q - 1
                    to_mid(j).wait_recv()
                    mine[j] = mine[j] + edge[j]
                    across(j).start()

                @pl.when((q >= 1 + RB_LAG) & (q < pieces + 1 + RB_LAG))
                def _():
                    j = q - 1 - RB_LAG
                    across(j).wait_recv()
                    r, half, cols = place(j)
                    at = pl.ds(pl.multiple_of(r * OWN + half * PIECE, PIECE), PIECE)
                    val = own_ref[at, cols].astype(jnp.float32) + (mine[j] + cross[j])
                    val = val.astype(jnp.bfloat16).astype(jnp.float32)
                    edge[j] = val
                    to_end(j).start()
                    result(j, val, None)
                    across(j).wait_send()
                    if last:
                        to_far(j).start()
                        to_near(j).start()

            if last:
                @pl.when((q >= Y_LAG) & (q < pieces + Y_LAG))
                def _():
                    j = q - Y_LAG
                    to_far(j).wait_recv()
                    hand_on(j).start()
                    foreign(j, from_y[j], (sp + 2) % 4)
                    to_near(j).wait_recv()
                    foreign(j, from_c[j], sp + 1 - 2 * (sp % 2))

                @pl.when(q >= Y_LAG + B_LAG)
                def _():
                    j = q - Y_LAG - B_LAG
                    hand_on(j).wait_recv()
                    foreign(j, from_b[j], (sp + 3 - 2 * (sp % 2)) % 4)
            return 0

        steps = pieces + (Y_LAG + B_LAG if last else END_LAG)
        lax.fori_loop(0, steps, step, 0)

        def drain(j, _):
            @pl.when(is_mid)
            def _():
                to_end(j).wait_send()

            if last:
                to_far(j).wait_send()
                to_near(j).wait_send()
                hand_on(j).wait_send()
            return 0

        lax.fori_loop(0, pieces, drain, 0)

    f32, bf16 = jnp.float32, jnp.bfloat16
    dma = pltpu.SemaphoreType.DMA
    buf = pltpu.VMEM((pieces, PIECE, COLS), f32)
    scratch = [
        pltpu.VMEM((WSLOTS, width, COLS), bf16),
        pltpu.VMEM((WSLOTS, inner, COLS), bf16),
        dma((WSLOTS, 2)),
        buf, buf, buf,
    ] + [dma((pieces,))] * 5
    if last:
        scratch += [buf] * 3 + [dma((pieces,))] * 6
        out = jax.ShapeDtypeStruct((rows, CHUNK, model), bf16)
    else:
        out = jax.ShapeDtypeStruct((tokens, model), bf16)
    vmem = pl.BlockSpec(memory_space=pltpu.VMEM)
    hbm = pl.BlockSpec(memory_space=pl.ANY)
    return pl.pallas_call(
        kernel,
        in_specs=[vmem, vmem, vmem, hbm, hbm],
        out_specs=vmem,
        out_shape=out,
        scratch_shapes=scratch,
        compiler_params=pltpu.CompilerParams(collective_id=layer, has_side_effects=True, vmem_limit_bytes=60 << 20),
        cost_estimate=pl.CostEstimate(flops=2 * tokens * model * (width + inner), transcendentals=0, bytes_accessed=60 << 20),
        name="line_sum_last" if last else "line_sum",
    )(att, mid, own, w_out, w_down)


def local_step(x, prior_len, ln_gain, w_query, w_key, w_value, w_out, w_gate, w_up, w_down, swa_k, swa_v, glb_k, glb_v):
    rows = x.shape[0]
    sp = lax.axis_index('sp')
    prior = prior_len.astype(jnp.int32)
    flat = lambda c: c.reshape(rows, -1, HEAD_DIM)
    sk, sv, gk, gv = flat(swa_k), flat(swa_v), flat(glb_k), flat(glb_v)
    me = jnp.stack([sp]).astype(jnp.int32)
    side = jnp.stack([lax.div(sp, 2)]).astype(jnp.int32)

    def middle(h, layer):
        return (jax.nn.silu(dot32(h, w_gate[layer])) * dot32(h, w_up[layer])).astype(jnp.bfloat16)

    own, fresh_k, fresh_v = norm_and_keys(me, x, ln_gain[0:1], w_key[0], w_value[0])
    q = dot32(own, w_query[0]).astype(jnp.bfloat16)
    mid = middle(own, 0)
    swa = None
    parts = []
    for b in range(rows):
        cosine, sine = rope_tables(prior[b])
        info = jnp.stack([lax.rem(prior[b], WINDOW), sp * OWN]).astype(jnp.int32)
        tok = slice(b * OWN, (b + 1) * OWN)
        chunk = slice(b * CHUNK, (b + 1) * CHUNK)
        att, *swa = attention(b, False, info, (q[tok], fresh_k[chunk], fresh_v[chunk], cosine, sine), sk, sv, swa)
        parts.append(att)
    x_own = lax.dynamic_slice_in_dim(x, sp * OWN, OWN, axis=1).reshape(rows * OWN, -1)
    hidden = line_sum(False, 0, jnp.concatenate(parts, axis=0), mid, x_own, w_out, w_down, rows)

    h = layer_norm(hidden, ln_gain[1])
    qkv = jnp.concatenate([dot32(h, w_query[1]), dot32(h, w_key[1]), dot32(h, w_value[1])], axis=1)
    fars, nears, boths = [], [], []
    owns = [qkv[b * OWN:(b + 1) * OWN] for b in range(rows)]
    for b in range(rows):
        with scope(f"gyr{b}"):
            fars.append(swap(owns[b], 2))
        with scope(f"gnr{b}"):
            nears.append(swap(owns[b], 1))
    for b in range(rows):
        with scope(f"gbr{b}"):
            boths.append(swap(fars[b], 1))
    mid = middle(h, 1)
    glb = None
    parts = []
    for b in range(rows):
        info = jnp.stack([prior[b] - (sp * SHARD), lax.rem(sp, 2), sp]).astype(jnp.int32)
        with scope(f"at1r{b}"):
            keep, send, *glb = attention(b, True, info, (owns[b], fars[b], nears[b], boths[b]), gk, gv, glb)
        with scope(f"cnr{b}"):
            recv = swap(send, 1)
        with scope(f"mcr{b}"):
            keep, send = merge_cores(side, keep, recv)
        with scope(f"cyr{b}"):
            recv = swap(send, 2)
        with scope(f"mlr{b}"):
            parts.append(merge_last(keep, recv))
    result = line_sum(True, 1, jnp.concatenate(parts, axis=0), mid, hidden, w_out, w_down, rows)

    back = lambda c, like: c.reshape(like.shape)
    return result, back(swa[0], swa_k), back(swa[1], swa_v), back(glb[0], glb_k), back(glb[1], glb_v)


def solution(mesh):
    col_spec = P(None, None, 'tp')
    row_spec = P(None, 'tp', None)
    swa_spec = P('dp', None, 'tp', None)
    glb_spec = P('dp', 'sp', 'tp', None)
    in_specs = (P('dp', None, None), P('dp'), P(None, None), col_spec, col_spec, col_spec, row_spec,
                col_spec, col_spec, row_spec, swa_spec, swa_spec, glb_spec, glb_spec)
    out_specs = (P('dp', None, None), swa_spec, swa_spec, glb_spec, glb_spec)
    return jax.shard_map(local_step, mesh=mesh, in_specs=in_specs, out_specs=out_specs, check_vma=False)
```

```python
import functools
import math

import jax
import jax.numpy as jnp
from jax import lax
from jax.experimental import pallas as pl
from jax.experimental.pallas import tpu as pltpu
from jax.sharding import PartitionSpec as P

HEAD_DIM = 128
ROPE_BASE = 50000
NORM_EPS = 1e-5
WINDOW = 4096
SHARD = 4096
CHUNK = 512
OWN = 128
BK = 1024
NEG = -1e30
LOG2E_SCALE = math.log2(math.e) / math.sqrt(HEAD_DIM)
MESH = pl.DeviceIdType.MESH


def layer_norm(hidden, norm_gain):
    as_float = hidden.astype(jnp.float32)
    centered = as_float - jnp.mean(as_float, axis=-1, keepdims=True)
    variance = jnp.mean(centered * centered, axis=-1, keepdims=True)
    return (centered * lax.rsqrt(variance + NORM_EPS) * norm_gain.astype(jnp.float32)).astype(jnp.bfloat16)


def rope_tables(prior):
    lane = lax.broadcasted_iota(jnp.int32, (1, HEAD_DIM), 1)
    inv_freq = ROPE_BASE ** (-((lane // 2) * 2).astype(jnp.float32) / HEAD_DIM)
    positions = (prior[:, None] + jnp.arange(CHUNK, dtype=jnp.int32)[None, :]).astype(jnp.float32).reshape(-1)
    angles = positions[:, None] * inv_freq
    return jnp.cos(angles), jnp.where(lane % 2 == 0, -jnp.sin(angles), jnp.sin(angles))


def rotate(vec, cosine, sine):
    lane = lax.broadcasted_iota(jnp.int32, vec.shape, 1)
    swapped = jnp.where(lane % 2 == 0, pltpu.roll(vec, HEAD_DIM - 1, 1), pltpu.roll(vec, 1, 1))
    return vec * cosine + swapped * sine


class Tiles:
    def __init__(self, qt, acc, mx, sm, alpha, s0, s1, p0, p1, tick=None):
        self.qt, self.acc, self.mx, self.sm, self.alpha = qt, acc, mx, sm, alpha
        self.s, self.p, self.tick = (s0, s1), (p0, p1), tick
        self.tiles = qt.shape[0]

    def reset(self):
        self.mx[...] = jnp.full_like(self.mx, NEG)
        self.sm[...] = jnp.zeros_like(self.sm)
        self.acc[...] = jnp.zeros_like(self.acc)

    def process(self, nk, k_src, vt_src, mask_fn, first_tick=0):
        per_g = self.tiles // 2

        def tile_g(t):
            return t // per_g if per_g > 1 else t

        def qk(t, slot):
            s = jnp.dot(k_src[tile_g(t), :nk, :], self.qt[t], preferred_element_type=jnp.float32)
            if mask_fn is not None:
                s = jnp.where(mask_fn(t, nk), s, NEG)
            self.s[slot][:nk, :] = s
            self.alpha[slot, 1:2, :] = jnp.max(s, axis=0, keepdims=True)

        def soft(t, slot):
            old = self.mx[t, 0:1, :]
            new = jnp.maximum(old, self.alpha[slot, 1:2, :])
            e = jnp.exp2((self.s[slot][:nk, :] - new) * LOG2E_SCALE)
            fade = jnp.exp2((old - new) * LOG2E_SCALE)
            self.sm[t, 0:1, :] = self.sm[t, 0:1, :] * fade + jnp.sum(e, axis=0, keepdims=True)
            self.mx[t, 0:1, :] = new
            self.alpha[slot, 0:1, :] = fade
            self.p[slot][:nk, :] = e.astype(jnp.bfloat16)

        def pv(t, slot):
            add = jnp.dot(vt_src[tile_g(t), :, :nk], self.p[slot][:nk, :], preferred_element_type=jnp.float32)
            self.acc[t] = self.acc[t] * self.alpha[slot, 0:1, :] + add

        qk(0, 0)
        qk(1, 1)
        soft(0, 0)
        pairs = self.tiles // 2
        if pairs > 1:
            def body(i, _):
                t = 2 * i
                qk(t + 2, 0)
                soft(t + 1, 1)
                pv(t, 0)
                qk(t + 3, 1)
                soft(t + 2, 0)
                pv(t + 1, 1)
                if self.tick is not None:
                    self.tick(first_tick + i)
                return 0

            lax.fori_loop(0, pairs - 1, body, 0)
        soft(self.tiles - 1, 1)
        pv(self.tiles - 2, 0)
        pv(self.tiles - 1, 1)
        if self.tick is not None:
            self.tick(first_tick + pairs - 1)


def split_heads(k, v, inter, kg, vt):
    inter[...] = k.astype(jnp.float32)
    for g in range(2):
        kg[g] = inter[pl.ds(g, BK, stride=2), :].astype(jnp.bfloat16)
    inter[...] = v.astype(jnp.float32)
    for g in range(2):
        vt[g] = inter[pl.ds(g, BK, stride=2), :].T.astype(jnp.bfloat16)


def sliding_attention(place, q, fresh_k, fresh_v, cosine, sine, swa_k, swa_v, glb_k, glb_v):
    rows = swa_k.shape[0]
    width = 3 * OWN

    def kernel(place_ref, q_ref, k_ref, v_ref, cos_ref, sin_ref, kc_ref, vc_ref, gk_ref, gv_ref, att_ref, ko_ref, vo_ref,
               gko_ref, gvo_ref, qt, acc, mx, sm, alpha, inter, kg, vt, fk, fvt, padk, padv, s0, s1, p0, p1):
        row, step = pl.program_id(0), pl.program_id(1)
        slot_first = lax.rem(place_ref[row], WINDOW)
        first_tok = place_ref[3] * OWN
        heads = Tiles(qt, acc, mx, sm, alpha, s0, s1, p0, p1)
        gko_ref[0] = gk_ref[0]
        gvo_ref[0] = gv_ref[0]
        token = lax.rem(lax.broadcasted_iota(jnp.int32, (1, width), 1), OWN) + first_tok

        @pl.when(step == 0)
        def _():
            heads.reset()
            at = pl.ds(pl.multiple_of(first_tok, OWN), OWN)
            for h in range(6):
                g, j = divmod(h, 3)
                val = q_ref[:, h * HEAD_DIM:(h + 1) * HEAD_DIM].astype(jnp.float32)
                val = rotate(val, cos_ref[at, :], sin_ref[at, :])
                qt[g, :, j * OWN:(j + 1) * OWN] = val.T.astype(jnp.bfloat16)
            for g in range(2):
                for b in range(4):
                    rows_b = slice(b * OWN, (b + 1) * OWN)
                    cols = slice(g * HEAD_DIM, (g + 1) * HEAD_DIM)
                    kval = rotate(k_ref[rows_b, cols].astype(jnp.float32), cos_ref[rows_b, :], sin_ref[rows_b, :])
                    kval = kval.astype(jnp.bfloat16)
                    vval = v_ref[rows_b, cols].astype(jnp.float32)
                    spread = pl.ds(2 * BK + 2 * b * OWN + g, OWN, stride=2)
                    padk[spread, :] = kval.astype(jnp.float32)
                    padv[spread, :] = vval
                    fk[g, rows_b, :] = kval
                    fvt[g, :, rows_b] = vval.T.astype(jnp.bfloat16)
            heads.process(CHUNK, fk, fvt,
                          lambda t, nk: lax.broadcasted_iota(jnp.int32, (nk, width), 0) <= token)

        shift = step * BK - slot_first
        shift = jnp.where(shift >= WINDOW // 2, shift - WINDOW, shift)
        shift = jnp.where(shift < -(WINDOW // 2), shift + WINDOW, shift)
        touched = (shift > -BK) & (shift < CHUNK)

        @pl.when(jnp.logical_not(touched))
        def _():
            ko_ref[0] = kc_ref[0]
            vo_ref[0] = vc_ref[0]

        @pl.when(touched)
        def _():
            fresh = lax.broadcasted_iota(jnp.int32, (2 * BK, 1), 0) // 2 + shift
            inside = (fresh >= 0) & (fresh < CHUNK)
            at = pl.ds(2 * BK + 2 * shift, 2 * BK)
            ko_ref[0] = jnp.where(inside, padk[at, :], kc_ref[0].astype(jnp.float32)).astype(jnp.bfloat16)
            vo_ref[0] = jnp.where(inside, padv[at, :], vc_ref[0].astype(jnp.float32)).astype(jnp.bfloat16)

        def old_mask(t, nk):
            fresh = lax.broadcasted_iota(jnp.int32, (nk, width), 0) + shift
            return (fresh < 0) | (fresh > token)

        split_heads(kc_ref[0], vc_ref[0], inter, kg, vt)

        @pl.when(touched)
        def _():
            heads.process(BK, kg, vt, old_mask)

        @pl.when(jnp.logical_not(touched))
        def _():
            heads.process(BK, kg, vt, None)

        @pl.when(step == pl.num_programs(1) - 1)
        def _():
            for g in range(2):
                for j in range(3):
                    cols = slice(j * OWN, (j + 1) * OWN)
                    h = 3 * g + j
                    att_ref[:, h * HEAD_DIM:(h + 1) * HEAD_DIM] = (acc[g, :, cols] / sm[g, 0:1, cols]).T.astype(jnp.bfloat16)

    f32, bf16 = jnp.float32, jnp.bfloat16
    per_row = lambda n, w: pl.BlockSpec((n, w), lambda r, i, place: (r, 0))
    cache = pl.BlockSpec((1, 2 * BK, HEAD_DIM), lambda r, i, place: (r, i, 0))
    keys = WINDOW + CHUNK
    return pl.pallas_call(
        kernel,
        grid_spec=pltpu.PrefetchScalarGridSpec(
            num_scalar_prefetch=1,
            grid=(rows, WINDOW // BK),
            in_specs=[per_row(OWN, 6 * HEAD_DIM), per_row(CHUNK, 2 * HEAD_DIM), per_row(CHUNK, 2 * HEAD_DIM),
                      per_row(CHUNK, HEAD_DIM), per_row(CHUNK, HEAD_DIM)] + [cache] * 4,
            out_specs=[per_row(OWN, 6 * HEAD_DIM)] + [cache] * 4,
            scratch_shapes=[
                pltpu.VMEM((2, HEAD_DIM, width), bf16),
                pltpu.VMEM((2, HEAD_DIM, width), f32),
                pltpu.VMEM((2, 8, width), f32),
                pltpu.VMEM((2, 8, width), f32),
                pltpu.VMEM((2, 8, width), f32),
                pltpu.VMEM((2 * BK, HEAD_DIM), f32),
                pltpu.VMEM((2, BK, HEAD_DIM), bf16),
                pltpu.VMEM((2, HEAD_DIM, BK), bf16),
                pltpu.VMEM((2, CHUNK, HEAD_DIM), bf16),
                pltpu.VMEM((2, HEAD_DIM, CHUNK), bf16),
                pltpu.VMEM((4 * BK + 2 * CHUNK, HEAD_DIM), f32),
                pltpu.VMEM((4 * BK + 2 * CHUNK, HEAD_DIM), f32),
                pltpu.VMEM((BK, width), f32),
                pltpu.VMEM((BK, width), f32),
                pltpu.VMEM((BK, width), bf16),
                pltpu.VMEM((BK, width), bf16),
            ],
        ),
        out_shape=[jax.ShapeDtypeStruct((rows * OWN, 6 * HEAD_DIM), bf16)]
        + [jax.ShapeDtypeStruct(c.shape, c.dtype) for c in (swa_k, swa_v, glb_k, glb_v)],
        compiler_params=pltpu.CompilerParams(dimension_semantics=("arbitrary", "arbitrary"), vmem_limit_bytes=48 << 20),
        cost_estimate=pl.CostEstimate(flops=8 * rows * width * keys * HEAD_DIM, transcendentals=2 * rows * width * keys,
                                      bytes_accessed=50 << 20),
        name="sliding_rows",
    )(place, q, fresh_k, fresh_v, cosine, sine, swa_k, swa_v, glb_k, glb_v)


WIN = CHUNK + 16
PAD = WIN


def patch_cache(place, own, far, near, both, result, cache_k, cache_v):
    rows = cache_k.shape[0]
    last = cache_k.shape[1] // 2 - WIN

    def kernel(place_ref, own_ref, far_ref, near_ref, both_ref, res_ref, k_in, v_in, out_ref, k_out, v_out, padk, padv, bufk, bufv,
               sems):
        del k_in, v_in
        out_ref[...] = res_ref[...]
        row, me = pl.program_id(0), place_ref[3]
        rel = place_ref[row] - me * SHARD

        @pl.when((rel > -CHUNK) & (rel < SHARD) & (pl.program_id(1) == 0))
        def _():
            first = jnp.clip(lax.div(rel + SHARD, 8) * 8 - SHARD, 0, last)
            at = pl.ds(pl.multiple_of(2 * first, 16), 2 * WIN)
            loads = [pltpu.make_async_copy(out.at[row, at, :], buf, sems.at[i])
                     for i, (out, buf) in enumerate(((k_out, bufk), (v_out, bufv)))]
            for copy in loads:
                copy.start()
            for src, block in ((own_ref[...], me), (far_ref[0], me ^ 2), (near_ref[0], me ^ 1), (both_ref[0], me ^ 3)):
                for g in range(2):
                    spread = pl.ds(2 * PAD + 2 * block * OWN + g, OWN, stride=2)
                    padk[spread, :] = src[:, (6 + g) * HEAD_DIM:(7 + g) * HEAD_DIM]
                    padv[spread, :] = src[:, (8 + g) * HEAD_DIM:(9 + g) * HEAD_DIM]
            for copy in loads:
                copy.wait()
            fresh = lax.broadcasted_iota(jnp.int32, (2 * WIN, 1), 0) // 2 + (first - rel)
            inside = (fresh >= 0) & (fresh < CHUNK)
            for i, (pad, buf, out) in enumerate(((padk, bufk, k_out), (padv, bufv, v_out))):
                new = pad[pl.ds(2 * PAD + 2 * (first - rel), 2 * WIN), :]
                buf[...] = jnp.where(inside, new, buf[...].astype(jnp.float32)).astype(jnp.bfloat16)
                pltpu.make_async_copy(buf, out.at[row, at, :], sems.at[i]).start()
            for i, (buf, out) in enumerate(((bufk, k_out), (bufv, v_out))):
                pltpu.make_async_copy(buf, out.at[row, at, :], sems.at[i]).wait()

    piece = pl.BlockSpec((1, OWN, own.shape[1]), lambda r, i, place: (r, 0, 0))
    block = pl.BlockSpec((1, OWN, result.shape[2]), lambda r, i, place: (r, i, 0))
    hbm = pl.BlockSpec(memory_space=pl.ANY)
    pad = pltpu.VMEM((4 * PAD + 2 * CHUNK, HEAD_DIM), jnp.float32)
    buf = pltpu.VMEM((2 * WIN, HEAD_DIM), jnp.bfloat16)
    return pl.pallas_call(
        kernel,
        grid_spec=pltpu.PrefetchScalarGridSpec(
            num_scalar_prefetch=1,
            grid=(rows, CHUNK // OWN),
            in_specs=[pl.BlockSpec((OWN, own.shape[1]), lambda r, i, place: (r, 0)), piece, piece, piece, block, hbm, hbm],
            out_specs=[block, hbm, hbm],
            scratch_shapes=[pad, pad, buf, buf, pltpu.SemaphoreType.DMA((2,))],
        ),
        out_shape=[jax.ShapeDtypeStruct(c.shape, c.dtype) for c in (result, cache_k, cache_v)],
        input_output_aliases={6: 1, 7: 2},
        compiler_params=pltpu.CompilerParams(dimension_semantics=("arbitrary", "arbitrary")),
        cost_estimate=pl.CostEstimate(flops=1 << 30, transcendentals=0, bytes_accessed=10 << 20),
        name="patch_cache",
    )(place, own, far, near, both, result, cache_k, cache_v)


def merge_pair(a, b, normalise):
    lane = lax.broadcasted_iota(jnp.int32, (a.shape[0], HEAD_DIM), 1)
    sa, sb = a[:, 6 * HEAD_DIM:], b[:, 6 * HEAD_DIM:]
    stats = jnp.zeros_like(sa)
    heads = []
    for h in range(6):
        ma, mb = sa[:, h:h + 1], sb[:, h:h + 1]
        la, lb = sa[:, 8 + h:9 + h], sb[:, 8 + h:9 + h]
        top = jnp.maximum(ma, mb)
        fa, fb = jnp.exp2(ma - top), jnp.exp2(mb - top)
        total = la * fa + lb * fb
        cols = slice(h * HEAD_DIM, (h + 1) * HEAD_DIM)
        val = a[:, cols] * fa + b[:, cols] * fb
        if normalise:
            val = val / total
        heads.append(val)
        stats = jnp.where(lane == h, top, jnp.where(lane == 8 + h, total, stats))
    return heads, stats


def norm_and_keys(me, x, gain, w_key, w_value):
    rows, chunk, model = x.shape
    kv = w_key.shape[2]
    parts = 2
    steps = chunk // (parts * OWN)

    def kernel(me_ref, x_ref, gain_ref, wk_hbm, wv_hbm, own_ref, k_ref, v_ref, wkv, h0, h1, sems):
        first = (pl.program_id(0) == 0) & (pl.program_id(1) == 0)
        loads = [pltpu.make_async_copy(w.at[0], wkv.at[:, pl.ds(i * kv, kv)], sems.at[i]) for i, w in enumerate((wk_hbm, wv_hbm))]

        @pl.when(first)
        def _():
            for copy in loads:
                copy.start()

        h0[...] = layer_norm(x_ref[0, :OWN], gain_ref[0:1, :])

        @pl.when(first)
        def _():
            for copy in loads:
                copy.wait()

        both = jnp.dot(h0[...], wkv[...], preferred_element_type=jnp.float32).astype(jnp.bfloat16)
        h1[...] = layer_norm(x_ref[0, OWN:], gain_ref[0:1, :])
        k_ref[:OWN] = both[:, :kv]
        v_ref[:OWN] = both[:, kv:]
        both = jnp.dot(h1[...], wkv[...], preferred_element_type=jnp.float32).astype(jnp.bfloat16)
        k_ref[OWN:] = both[:, :kv]
        v_ref[OWN:] = both[:, kv:]
        for i, h in enumerate((h0, h1)):
            @pl.when(pl.program_id(1) * parts + i == me_ref[0])
            def _(h=h):
                own_ref[...] = h[...]

    hbm = pl.BlockSpec(memory_space=pl.ANY)
    per_step = pl.BlockSpec((parts * OWN, kv), lambda r, i, me: (r * steps + i, 0))
    return pl.pallas_call(
        kernel,
        grid_spec=pltpu.PrefetchScalarGridSpec(
            num_scalar_prefetch=1,
            grid=(rows, steps),
            in_specs=[
                pl.BlockSpec((1, parts * OWN, model), lambda r, i, me: (r, i, 0)),
                pl.BlockSpec((2, model), lambda r, i, me: (0, 0)),
                hbm, hbm,
            ],
            out_specs=[pl.BlockSpec((OWN, model), lambda r, i, me: (r, 0)), per_step, per_step],
            scratch_shapes=[pltpu.VMEM((model, 2 * kv), jnp.bfloat16), pltpu.VMEM((OWN, model), jnp.bfloat16),
                            pltpu.VMEM((OWN, model), jnp.bfloat16), pltpu.SemaphoreType.DMA((2,))],
        ),
        out_shape=[
            jax.ShapeDtypeStruct((rows * OWN, model), jnp.bfloat16),
            jax.ShapeDtypeStruct((rows * chunk, kv), jnp.bfloat16),
            jax.ShapeDtypeStruct((rows * chunk, kv), jnp.bfloat16),
        ],
        compiler_params=pltpu.CompilerParams(dimension_semantics=("arbitrary", "arbitrary"), vmem_limit_bytes=58 << 20),
        cost_estimate=pl.CostEstimate(flops=4 * rows * chunk * model * kv, transcendentals=0, bytes_accessed=16 << 20),
        name="norm_and_keys",
    )(me, x, gain, w_key, w_value)


WSLOTS = 3
RB_LAG = 3
END_LAG = 9
GCOLS = 256


class Line:
    def __init__(self, mine, edge, cross, s1, r1, s2, r2, s3):
        self.mine, self.edge, self.cross = mine, edge, cross
        self.sems = s1, r1, s2, r2, s3
        tp = lax.axis_index("tp")
        self.is_mid = (tp == 1) | (tp == 2)
        self.is_end = (tp == 0) | (tp == 3)
        self.inward = {"tp": 1 + tp // 3}
        self.outward = {"tp": 3 * (tp // 2)}
        self.partner = {"tp": 3 - tp}

    def to_mid(self, j):
        s1, r1, *_ = self.sems
        return remote(self.mine.at[j], self.edge.at[j], s1.at[j], r1.at[j], self.inward)

    def across(self, j):
        _, _, s2, r2, _ = self.sems
        return remote(self.mine.at[j], self.cross.at[j], s2.at[j], r2.at[j], self.partner)

    def to_end(self, j):
        _, r1, _, _, s3 = self.sems
        return remote(self.edge.at[j], self.edge.at[j], s3.at[j], r1.at[j], self.outward)

    def meet(self, others):
        barrier = pltpu.get_barrier_semaphore()

        def signal(to):
            pl.semaphore_signal(barrier, inc=1, device_id=to, device_id_type=MESH)

        for to in others:
            signal(to)

        @pl.when(self.is_end)
        def _():
            signal(self.inward)
            pl.semaphore_wait(barrier, 1 + len(others))

        @pl.when(self.is_mid)
        def _():
            signal(self.outward)
            signal(self.partner)
            pl.semaphore_wait(barrier, 2 + len(others))

    def step(self, q, pieces, own_of, done):
        @pl.when(self.is_end)
        def _():
            @pl.when((q >= 4) & (q < pieces + 4))
            def _():
                self.to_mid(q - 4).wait_send()

            @pl.when(q < pieces)
            def _():
                self.to_mid(q).start()

            @pl.when((q >= END_LAG) & (q < pieces + END_LAG))
            def _():
                j = q - END_LAG
                self.to_end(j).wait_recv()
                done(j, self.edge[j])

        @pl.when(self.is_mid)
        def _():
            @pl.when((q >= 1) & (q < pieces + 1))
            def _():
                j = q - 1
                self.to_mid(j).wait_recv()
                self.mine[j] = self.mine[j] + self.edge[j]
                self.across(j).start()

            @pl.when((q >= 1 + RB_LAG) & (q < pieces + 1 + RB_LAG))
            def _():
                j = q - 1 - RB_LAG
                self.across(j).wait_recv()
                val = own_of(j) + (self.mine[j] + self.cross[j])
                val = val.astype(jnp.bfloat16).astype(jnp.float32)
                self.edge[j] = val
                self.to_end(j).start()
                done(j, val)
                self.across(j).wait_send()


def remote(src, dst, send, recv, to):
    return pltpu.make_async_remote_copy(src, dst, send, recv, device_id=to, device_id_type=MESH)


MLP_AT = (2, 12, 22, 34)
NORM_AT = 21


def layer_end(att, normed, x, gain, w_query, w_key, w_value, w_out, w_gate, w_up, w_down):
    rows, _, model = x.shape
    tokens = rows * OWN
    width, inner, kv = att.shape[1], w_gate.shape[2], w_key.shape[2]
    qkv = width + 2 * kv
    ncol, nmlp = model // GCOLS, inner // GCOLS
    pieces = rows * ncol
    chunks = 2 * rows * nmlp

    def kernel(att_ref, h_ref, gain_ref, x_hbm, wq_hbm, wk_hbm, wv_hbm, wo_hbm, wg_hbm, wu_hbm, wd_hbm,
               hid_ref, qkv_ref, mid1_ref, far_q, near_q, both_q,
               own_x, mid0, wqkv, wg, wu, wo, wd, h1, mine, edge, cross,
               xsem, qsem, gsem, wsem, gs, gr, s1, r1, s2, r2, s3):
        sp = lax.axis_index("sp")
        core = sp % 2
        far, near = {"sp": (sp + 2) % 4}, {"sp": sp + 1 - 2 * core}
        line = Line(mine, edge, cross, s1, r1, s2, r2, s3)

        def rows_of(r):
            return pl.ds(pl.multiple_of(r * OWN, OWN), OWN)

        def cols_of(n):
            return pl.ds(pl.multiple_of(n * GCOLS, GCOLS), GCOLS)

        def x_copies():
            return [pltpu.make_async_copy(x_hbm.at[r, rows_of(sp), :], own_x.at[r], xsem.at[r]) for r in range(rows)]

        def qkv_copies():
            return [pltpu.make_async_copy(w.at[1], wqkv.at[:, pl.ds(at, n)], qsem.at[i])
                    for i, (w, at, n) in enumerate(((wq_hbm, 0, width), (wk_hbm, width, kv), (wv_hbm, width + kv, kv)))]

        def mlp_copies(c):
            layer, n, slot = c // (rows * nmlp), c % nmlp, c % WSLOTS
            return (pltpu.make_async_copy(wg_hbm.at[layer, :, cols_of(n)], wg.at[slot], gsem.at[slot, 0]),
                    pltpu.make_async_copy(wu_hbm.at[layer, :, cols_of(n)], wu.at[slot], gsem.at[slot, 1]))

        def out_copies(j):
            slot = j % WSLOTS
            return (pltpu.make_async_copy(wo_hbm.at[0, :, cols_of(j % ncol)], wo.at[slot], wsem.at[slot, 0]),
                    pltpu.make_async_copy(wd_hbm.at[0, :, cols_of(j % ncol)], wd.at[slot], wsem.at[slot, 1]))

        def q_far():
            return remote(qkv_ref.at[pl.ds(0, OWN)], far_q, gs.at[0], gr.at[0], far)

        def q_near():
            return remote(qkv_ref.at[pl.ds(0, OWN)], near_q, gs.at[1], gr.at[1], near)

        def q_both():
            return remote(far_q, both_q, gs.at[2], gr.at[2], near)

        def mlp(c):
            slot, n = c % WSLOTS, c % nmlp
            r = (c // nmlp) % rows
            for copy in mlp_copies(c):
                copy.wait()

            def middle(h):
                gate = jnp.dot(h, wg[slot], preferred_element_type=jnp.float32)
                return (jax.nn.silu(gate) * jnp.dot(h, wu[slot], preferred_element_type=jnp.float32)).astype(jnp.bfloat16)

            @pl.when(c < rows * nmlp)
            def _():
                mid0[rows_of(r), cols_of(n)] = middle(h_ref[rows_of(r), :])

            @pl.when(c >= rows * nmlp)
            def _():
                mid1_ref[rows_of(r), cols_of(n)] = middle(h1[...])

            @pl.when(c + WSLOTS < chunks)
            def _():
                for copy in mlp_copies(c + WSLOTS):
                    copy.start()

        def project(r):
            h1[...] = layer_norm(hid_ref[rows_of(r), :], gain_ref[1:2, :])
            for n in range(qkv // GCOLS):
                cols = slice(n * GCOLS, (n + 1) * GCOLS)
                qkv_ref[rows_of(r), cols] = jnp.dot(h1[...], wqkv[:, cols], preferred_element_type=jnp.float32)

        def own_of(j):
            return own_x[j // ncol, :, cols_of(j % ncol)].astype(jnp.float32)

        def done(j, val):
            hid_ref[rows_of(j // ncol), cols_of(j % ncol)] = val.astype(jnp.bfloat16)

        for c in range(WSLOTS):
            for copy in mlp_copies(c):
                copy.start()
        for j in range(WSLOTS):
            for copy in out_copies(j):
                copy.start()
        for copy in x_copies() + qkv_copies():
            copy.start()
        line.meet((far, near))

        def first(c, _):
            mlp(c)
            return 0

        lax.fori_loop(0, nmlp, first, 0)
        for copy in x_copies():
            copy.wait()

        def step(q, _):
            @pl.when(q < pieces)
            def _():
                slot, r = q % WSLOTS, q // ncol
                for copy in out_copies(q):
                    copy.wait()
                val = jnp.dot(att_ref[rows_of(r), :], wo[slot], preferred_element_type=jnp.float32)
                mine[q] = val + jnp.dot(mid0[rows_of(r), :], wd[slot], preferred_element_type=jnp.float32)

                @pl.when(q + WSLOTS < pieces)
                def _():
                    for copy in out_copies(q + WSLOTS):
                        copy.start()

            line.step(q, pieces, own_of, done)

            @pl.when(q == NORM_AT)
            def _():
                for copy in qkv_copies():
                    copy.wait()

            @pl.when((q >= NORM_AT) & ((q - NORM_AT) % ncol == 0))
            def _():
                project((q - NORM_AT) // ncol)

            @pl.when(q == NORM_AT)
            def _():
                q_far().start()
                q_near().start()

            @pl.when(q == NORM_AT + 7)
            def _():
                q_far().wait_recv()
                q_both().start()

            for i, at in enumerate(MLP_AT):
                @pl.when((q >= at) & (q < at + nmlp))
                def _(i=i, at=at):
                    mlp((i + 1) * nmlp + q - at)
            return 0

        lax.fori_loop(0, pieces + END_LAG, step, 0)
        project(rows - 1)

        def rest(c, _):
            mlp(c)
            return 0

        lax.fori_loop(chunks - nmlp, chunks, rest, 0)

        def drain(j, _):
            @pl.when(line.is_mid)
            def _():
                line.to_end(j).wait_send()
            return 0

        lax.fori_loop(0, pieces, drain, 0)
        q_near().wait_recv()
        q_both().wait_recv()
        for copy in (q_far(), q_near(), q_both()):
            copy.wait_send()

    f32, bf16 = jnp.float32, jnp.bfloat16
    dma = pltpu.SemaphoreType.DMA
    vm = pltpu.VMEM
    buf = vm((pieces, OWN, GCOLS), f32)
    vmem = pl.BlockSpec(memory_space=pltpu.VMEM)
    hbm = pl.BlockSpec(memory_space=pl.ANY)
    gathered = jax.ShapeDtypeStruct((OWN, qkv), f32)
    return pl.pallas_call(
        kernel,
        in_specs=[vmem, vmem, vmem] + [hbm] * 8,
        out_specs=[vmem] * 6,
        out_shape=[jax.ShapeDtypeStruct((tokens, model), bf16), jax.ShapeDtypeStruct((tokens, qkv), f32),
                   jax.ShapeDtypeStruct((tokens, inner), bf16), gathered, gathered, gathered],
        scratch_shapes=[
            vm((rows, OWN, model), bf16), vm((tokens, inner), bf16), vm((model, qkv), bf16),
            vm((WSLOTS, model, GCOLS), bf16), vm((WSLOTS, model, GCOLS), bf16),
            vm((WSLOTS, width, GCOLS), bf16), vm((WSLOTS, inner, GCOLS), bf16),
            vm((OWN, model), bf16), buf, buf, buf,
            dma((rows,)), dma((3,)), dma((WSLOTS, 2)), dma((WSLOTS, 2)), dma((3,)), dma((3,)),
        ] + [dma((pieces,))] * 5,
        compiler_params=pltpu.CompilerParams(collective_id=0, has_side_effects=True, vmem_limit_bytes=62 << 20),
        cost_estimate=pl.CostEstimate(flops=6 * tokens * model * inner, transcendentals=0, bytes_accessed=200 << 20),
        name="layer_end",
    )(att, normed, gain, x, w_query, w_key, w_value, w_out, w_gate, w_up, w_down)


TICKS = 6
ROW_TICKS = 5 * TICKS
MERGE_AT, ATT_AT, PIECE_EVERY = 3, 13, 2
FIRST_PIECE = ROW_TICKS + ATT_AT + 1
Y_LAG = 12
B_LAG = 2


def global_layer(place, own, far0, near0, both0, cache_k, cache_v, mid, hidden, w_out, w_down, rows):
    tokens, model = hidden.shape
    qkv = own.shape[1]
    width, inner = 6 * HEAD_DIM, mid.shape[1]
    ncol = model // GCOLS
    pieces = rows * ncol
    blocks = SHARD // BK
    part = 7 * HEAD_DIM
    lanes = 256

    def kernel(place_ref, own_hbm, far0_hbm, near0_hbm, both0_hbm, kc_hbm, vc_hbm, mid_ref, hid_ref, wo_hbm, wd_hbm,
               y_ref, far_q, near_q, both_q,
               own_q, qt, acc, mx, sm, alpha, s0, s1, p0, p1, kbuf, vbuf, inter, kg, vt, fk, fvt,
               keep, send, recv, keep2, send2, recv2, att, wo, wd, mine, edge, cross, from_y, from_c, from_b, stage,
               own_sem, first_sem, kv_sem, wsem, out_sem,
               gsf, grf, gsn, grn, gsb, grb, ucs, ucr, uys, uyr, s1_, r1_, s2_, r2_, s3_, sy, ry, sc, rc, sb, rb):
        sp = lax.axis_index("sp")
        core, side = sp % 2, sp // 2
        far_id, near_id, both_id = (sp + 2) % 4, sp + 1 - 2 * core, (sp + 3 - 2 * core) % 4
        far, near = {"sp": far_id}, {"sp": near_id}
        line = Line(mine, edge, cross, s1_, r1_, s2_, r2_, s3_)

        def own_rows(r):
            return own_hbm.at[pl.ds(pl.multiple_of(r * OWN, OWN), OWN), :]

        def own_copy(r):
            return pltpu.make_async_copy(own_rows(r), own_q, own_sem)

        def first_copies():
            return [pltpu.make_async_copy(a, b.at[0], first_sem.at[i])
                    for i, (a, b) in enumerate(((far0_hbm, far_q), (near0_hbm, near_q), (both0_hbm, both_q)))]

        def q_far(r):
            return remote(own_rows(r), far_q.at[r], gsf.at[r], grf.at[r], far)

        def q_near(r):
            return remote(own_rows(r), near_q.at[r], gsn.at[r], grn.at[r], near)

        def q_both(r):
            return remote(far_q.at[r], both_q.at[r], gsb.at[r], grb.at[r], near)

        def kv_copies(i):
            r, blk, slot = i // blocks, i % blocks, i % 2
            at = pl.ds(pl.multiple_of(blk * 2 * BK, 2 * BK), 2 * BK)
            return (pltpu.make_async_copy(kc_hbm.at[r, at, :], kbuf.at[slot], kv_sem.at[slot, 0]),
                    pltpu.make_async_copy(vc_hbm.at[r, at, :], vbuf.at[slot], kv_sem.at[slot, 1]))

        def u_near(r):
            return remote(send, recv.at[r], ucs.at[r], ucr.at[r], near)

        def u_far(r):
            return remote(send2, recv2.at[r], uys.at[r], uyr.at[r], far)

        def weights(j):
            slot = j % WSLOTS
            cols = pl.ds(pl.multiple_of((j % ncol) * GCOLS, GCOLS), GCOLS)
            return (pltpu.make_async_copy(wo_hbm.at[1, :, cols], wo.at[slot], wsem.at[slot, 0]),
                    pltpu.make_async_copy(wd_hbm.at[1, :, cols], wd.at[slot], wsem.at[slot, 1]))

        def y_far(j):
            return remote(edge.at[j], from_y.at[j], sy.at[j], ry.at[j], far)

        def y_near(j):
            return remote(edge.at[j], from_c.at[j], sc.at[j], rc.at[j], near)

        def y_both(j):
            return remote(from_y.at[j], from_b.at[j], sb.at[j], rb.at[j], near)

        def cols_of(j):
            return pl.ds(pl.multiple_of((j % ncol) * GCOLS, GCOLS), GCOLS)

        def out_copy(kind, j, owner):
            at = pl.ds(pl.multiple_of(owner * OWN, OWN), OWN)
            return pltpu.make_async_copy(stage.at[kind, j % 2], y_ref.at[j // ncol, at, cols_of(j)],
                                         out_sem.at[kind, j % 2])

        owners = (sp, far_id, near_id, both_id)

        def put_out(kind, j, val):
            @pl.when(j >= 2)
            def _():
                out_copy(kind, j - 2, owners[kind]).wait()

            stage[kind, j % 2] = val.astype(jnp.bfloat16)
            out_copy(kind, j, owners[kind]).start()

        def merge_cores(r):
            u_near(r).wait_recv()
            for half in range(2):
                heads, stats = merge_pair(keep[half], recv[r, half], False)
                mine_half = side == half
                for dst, cond in ((keep2, mine_half), (send2, jnp.logical_not(mine_half))):
                    @pl.when(cond)
                    def _(dst=dst):
                        for h in range(6):
                            dst[:, h * HEAD_DIM:(h + 1) * HEAD_DIM] = heads[h]
                        dst[:, width:] = stats
            u_far(r).start()
            u_near(r).wait_send()

        def merge_last(r):
            u_far(r).wait_recv()
            heads, _ = merge_pair(keep2[...], recv2[r], True)
            for h in range(6):
                att[r, :, h * HEAD_DIM:(h + 1) * HEAD_DIM] = heads[h].astype(jnp.bfloat16)
            u_far(r).wait_send()

        def own_of(j):
            at = pl.ds(pl.multiple_of((j // ncol) * OWN, OWN), OWN)
            return hid_ref[at, cols_of(j)].astype(jnp.float32)

        def done(j, val):
            put_out(0, j, val)
            y_far(j).start()
            y_near(j).start()

        def piece(q):
            @pl.when(q < pieces)
            def _():
                slot, r = q % WSLOTS, q // ncol
                for copy in weights(q):
                    copy.wait()
                rows_at = pl.ds(pl.multiple_of(r * OWN, OWN), OWN)
                val = jnp.dot(att[r], wo[slot], preferred_element_type=jnp.float32)
                mine[q] = val + jnp.dot(mid_ref[rows_at, :], wd[slot], preferred_element_type=jnp.float32)

                @pl.when(q + WSLOTS < pieces)
                def _():
                    for copy in weights(q + WSLOTS):
                        copy.start()

            line.step(q, pieces, own_of, done)

            @pl.when((q >= Y_LAG) & (q < pieces + Y_LAG))
            def _():
                j = q - Y_LAG
                y_far(j).wait_recv()
                y_both(j).start()
                put_out(1, j, from_y[j])
                y_near(j).wait_recv()
                put_out(2, j, from_c[j])

            @pl.when(q >= Y_LAG + B_LAG)
            def _():
                j = q - Y_LAG - B_LAG
                y_both(j).wait_recv()
                put_out(3, j, from_b[j])

        def tick(g):
            for r, at in ((1, 17), (2, ROW_TICKS + 2)):
                @pl.when(g == at)
                def _(r=r):
                    q_far(r).wait_recv()
                    q_both(r).start()

            @pl.when((g >= ROW_TICKS) & (g % ROW_TICKS == MERGE_AT))
            def _():
                merge_cores(g // ROW_TICKS - 1)

            @pl.when((g >= ROW_TICKS) & (g % ROW_TICKS == ATT_AT))
            def _():
                merge_last(g // ROW_TICKS - 1)

            since = g - FIRST_PIECE

            @pl.when((since >= 0) & (since % ROW_TICKS < PIECE_EVERY * ncol) & (since % ROW_TICKS % PIECE_EVERY == 0))
            def _():
                piece(since // ROW_TICKS * ncol + since % ROW_TICKS // PIECE_EVERY)

        for copy in first_copies() + [own_copy(0), *kv_copies(0)]:
            copy.start()
        for j in range(WSLOTS):
            for copy in weights(j):
                copy.start()
        line.meet((far, near))
        for r in range(1, rows):
            q_far(r).start()
            q_near(r).start()

        tiles = Tiles(qt, acc, mx, sm, alpha, s0, s1, p0, p1, tick)
        key = lax.broadcasted_iota(jnp.int32, (BK, 1), 0)

        def row(r, _):
            own_copy(r).wait()

            @pl.when(r == 0)
            def _():
                for copy in first_copies():
                    copy.wait()

            @pl.when(r > 0)
            def _():
                q_near(r).wait_recv()
                q_both(r).wait_recv()

            tiles.reset()
            for src, owner in ((own_q, sp), (far_q.at[r], far_id), (near_q.at[r], near_id), (both_q.at[r], both_id)):
                half = owner // 2
                in_tile = pl.ds(pl.multiple_of((owner % 2) * OWN, OWN), OWN)
                in_chunk = pl.ds(pl.multiple_of(owner * OWN, OWN), OWN)
                for h in range(6):
                    g, j = divmod(h, 3)
                    qt[g * 6 + j * 2 + half, :, in_tile] = src[:, h * HEAD_DIM:(h + 1) * HEAD_DIM].T.astype(jnp.bfloat16)
                for g in range(2):
                    fk[g, in_chunk, :] = src[:, (6 + g) * HEAD_DIM:(7 + g) * HEAD_DIM].astype(jnp.bfloat16)
                    fvt[g, :, in_chunk] = src[:, (8 + g) * HEAD_DIM:(9 + g) * HEAD_DIM].T.astype(jnp.bfloat16)

            @pl.when(r + 1 < rows)
            def _():
                own_copy(r + 1).start()

            rel = place_ref[r] - sp * SHARD

            def block(blk, _):
                i = r * blocks + blk
                for copy in kv_copies(i):
                    copy.wait()

                @pl.when(i + 1 < rows * blocks)
                def _():
                    for copy in kv_copies(i + 1):
                        copy.start()

                split_heads(kbuf[i % 2], vbuf[i % 2], inter, kg, vt)
                left = rel - blk * BK
                tiles.process(BK, kg, vt, lambda t, nk: key < left, r * ROW_TICKS + blk * TICKS)
                return 0

            lax.fori_loop(0, blocks, block, 0)

            def fresh_mask(t, nk):
                chunk_key = lax.broadcasted_iota(jnp.int32, (nk, lanes), 0)
                token = lax.broadcasted_iota(jnp.int32, (1, lanes), 1) + (t % 2) * lanes
                here = chunk_key + rel
                return (chunk_key <= token) & (here >= 0) & (here < SHARD)

            tiles.process(CHUNK, fk, fvt, fresh_mask, r * ROW_TICKS + blocks * TICKS)

            row_id = lax.broadcasted_iota(jnp.int32, (HEAD_DIM, OWN), 0)
            for half in range(2):
                stats = [jnp.zeros((HEAD_DIM, OWN), jnp.float32) for _ in range(2)]
                for h in range(6):
                    g, j = divmod(h, 3)
                    t = g * 6 + j * 2 + half
                    vals = []
                    for c in range(2):
                        cols = slice(c * OWN, (c + 1) * OWN)
                        vals.append(acc[t, :, cols].T)
                        stats[c] = jnp.where(row_id == h, mx[t, 0:1, cols] * LOG2E_SCALE, stats[c])
                        stats[c] = jnp.where(row_id == 8 + h, sm[t, 0:1, cols], stats[c])
                    cols = slice(h * HEAD_DIM, (h + 1) * HEAD_DIM)
                    keep[half, :, cols] = jnp.where(core == 0, vals[0], vals[1])
                    send[half, :, cols] = jnp.where(core == 0, vals[1], vals[0])
                s_a, s_b = stats[0].T, stats[1].T
                keep[half, :, width:] = jnp.where(core == 0, s_a, s_b)
                send[half, :, width:] = jnp.where(core == 0, s_b, s_a)
            u_near(r).start()
            return 0

        lax.fori_loop(0, rows, row, 0)

        merge_cores(rows - 1)
        since = [g % ROW_TICKS for g in range(rows * ROW_TICKS - FIRST_PIECE)]
        begun = sum(g < PIECE_EVERY * ncol and g % PIECE_EVERY == 0 for g in since)

        def tail(q, _):
            @pl.when(q == (rows - 1) * ncol)
            def _():
                merge_last(rows - 1)

            piece(q)
            return 0

        lax.fori_loop(begun, pieces + Y_LAG + B_LAG, tail, 0)

        def drain(j, _):
            @pl.when(line.is_mid)
            def _():
                line.to_end(j).wait_send()

            y_far(j).wait_send()
            y_near(j).wait_send()
            y_both(j).wait_send()
            return 0

        lax.fori_loop(0, pieces, drain, 0)
        for r in range(1, rows):
            q_far(r).wait_send()
            q_near(r).wait_send()
            q_both(r).wait_send()
        for kind in range(4):
            for j in (pieces - 2, pieces - 1):
                out_copy(kind, j, owners[kind]).wait()

    f32, bf16 = jnp.float32, jnp.bfloat16
    dma = pltpu.SemaphoreType.DMA
    vm = pltpu.VMEM
    buf = vm((pieces, OWN, GCOLS), f32)
    vmem = pl.BlockSpec(memory_space=pltpu.VMEM)
    hbm = pl.BlockSpec(memory_space=pl.ANY)
    gathered = jax.ShapeDtypeStruct((rows, OWN, qkv), f32)
    keys = SHARD + CHUNK
    return pl.pallas_call(
        kernel,
        in_specs=[pl.BlockSpec(memory_space=pltpu.SMEM)] + [hbm] * 6 + [vmem, vmem, hbm, hbm],
        out_specs=[hbm, vmem, vmem, vmem],
        out_shape=[jax.ShapeDtypeStruct((rows, CHUNK, model), bf16), gathered, gathered, gathered],
        scratch_shapes=[
            vm((OWN, qkv), f32),
            vm((12, HEAD_DIM, lanes), bf16), vm((12, HEAD_DIM, lanes), f32),
            vm((12, 8, lanes), f32), vm((12, 8, lanes), f32), vm((2, 8, lanes), f32),
            vm((BK, lanes), f32), vm((BK, lanes), f32), vm((BK, lanes), bf16), vm((BK, lanes), bf16),
            vm((2, 2 * BK, HEAD_DIM), bf16), vm((2, 2 * BK, HEAD_DIM), bf16), vm((2 * BK, HEAD_DIM), f32),
            vm((2, BK, HEAD_DIM), bf16), vm((2, HEAD_DIM, BK), bf16),
            vm((2, CHUNK, HEAD_DIM), bf16), vm((2, HEAD_DIM, CHUNK), bf16),
            vm((2, OWN, part), f32), vm((2, OWN, part), f32), vm((rows, 2, OWN, part), f32),
            vm((OWN, part), f32), vm((OWN, part), f32), vm((rows, OWN, part), f32),
            vm((rows, OWN, width), bf16),
            vm((WSLOTS, width, GCOLS), bf16), vm((WSLOTS, inner, GCOLS), bf16),
            buf, buf, buf, buf, buf, buf,
            vm((4, 2, OWN, GCOLS), bf16),
            dma, dma((3,)), dma((2, 2)), dma((WSLOTS, 2)), dma((4, 2)),
        ] + [dma((rows,))] * 10 + [dma((pieces,))] * 11,
        compiler_params=pltpu.CompilerParams(collective_id=1, has_side_effects=True, vmem_limit_bytes=67043328),
        cost_estimate=pl.CostEstimate(flops=rows * 4 * 12 * lanes * keys * HEAD_DIM, transcendentals=rows * 12 * lanes * keys,
                                      bytes_accessed=80 << 20),
        name="global_layer",
    )(place, own, far0, near0, both0, cache_k, cache_v, mid, hidden, w_out, w_down)


def dot32(a, b):
    return jnp.dot(a, b, preferred_element_type=jnp.float32)


def local_step(x, prior_len, ln_gain, w_query, w_key, w_value, w_out, w_gate, w_up, w_down, swa_k, swa_v, glb_k, glb_v):
    rows = x.shape[0]
    sp = lax.axis_index('sp')
    prior = prior_len.astype(jnp.int32)
    flat = lambda c: c.reshape(rows, -1, HEAD_DIM)
    me = jnp.full((1,), sp, jnp.int32)
    place = jnp.concatenate([prior, me])

    own, fresh_k, fresh_v = norm_and_keys(me, x, ln_gain, w_key, w_value)
    q = dot32(own, w_query[0]).astype(jnp.bfloat16)
    cosine, sine = rope_tables(prior)
    att, swa_k_new, swa_v_new, gk, gv = sliding_attention(place, q, fresh_k, fresh_v, cosine, sine, flat(swa_k), flat(swa_v),
                                                          flat(glb_k), flat(glb_v))
    hidden, qkv, mid, far, near, both = layer_end(att, own, x, ln_gain, w_query, w_key, w_value, w_out, w_gate, w_up, w_down)
    result, far, near, both = global_layer(place, qkv, far, near, both, flat(glb_k), flat(glb_v), mid, hidden, w_out, w_down,
                                           rows)
    result, gk, gv = patch_cache(place, qkv, far, near, both, result, gk, gv)
    back = lambda c, like: c.reshape(like.shape)
    return result, back(swa_k_new, swa_k), back(swa_v_new, swa_v), back(gk, glb_k), back(gv, glb_v)


def solution(mesh):
    col_spec = P(None, None, 'tp')
    row_spec = P(None, 'tp', None)
    swa_spec = P('dp', None, 'tp', None)
    glb_spec = P('dp', 'sp', 'tp', None)
    in_specs = (P('dp', None, None), P('dp'), P(None, None), col_spec, col_spec, col_spec, row_spec,
                col_spec, col_spec, row_spec, swa_spec, swa_spec, glb_spec, glb_spec)
    out_specs = (P('dp', None, None), swa_spec, swa_spec, glb_spec, glb_spec)
    return jax.shard_map(local_step, mesh=mesh, in_specs=in_specs, out_specs=out_specs, check_vma=False)
```
